256 devices in a mesh: expert: 8 (over x, core), shard: 32 (over z, y).
Axes of the slice: x: 4, y: 4, z: 8, core: 2. Of those that a mesh axis runs over, the one named last changes fastest.
Arguments:
- w_gate: float32 [64, 2048, 1408], P('expert', 'shard'), may hold values from -0.25 to 0.25
- w_up: float32 [64, 2048, 1408], P('expert', 'shard'), may hold values from -0.25 to 0.25
- router_weight: float32 [2048, 64], P('shard', 'expert'), may hold values from -0.125 to 0.125
- router_gain: float32 [2048], P('shard'), may hold values from 0.25 to 1.75
Outputs:
- serve_gate: bfloat16 [64, 2048, 1408], P('expert', None, 'shard')
- serve_up: bfloat16 [64, 2048, 1408], P('expert', None, 'shard')
- scale_gate: float32 [64, 1408], P('expert', 'shard')
- scale_up: float32 [64, 1408], P('expert', 'shard')
- serve_router: bfloat16 [2048, 64], replicated
The draws below stay inside these ranges and needn't reach their ends.
All inputs are finite; a program needn't handle non-finite values. Where the reference program divides by a largest or mean magnitude, that divisor is 1e-20 or more.
Results may differ from the reference program's by a relative error of at most 0.001.
Values may be sent and summed in bfloat16 or wider, within the bound.
No kernel may reach another device: no remote copies, remote signals or barrier semaphores. Data moves between devices by JAX's collectives and lax.ppermute only.
A program may use at most 64 MiB of HBM per device.

```python
import jax
import jax.numpy as jnp

EXPERTS = 64
D_MODEL = 2048
D_EXPERT = 1408


def raised(result, key, source, target, parts, factor):
    owner, partner = [(jnp.arange(result.shape[dim]) // (result.shape[dim] // parts)).reshape([-1 if axis == dim else 1 for axis in range(result.ndim)]) for dim in (source, target)]
    chosen = jax.random.permutation(key, parts)[partner]
    strong = (owner == chosen) | (owner == (partner + parts // 2) % parts)
    return jnp.where(strong, factor * result, result)


def block_levels(rng, shape, split, least, high):
    factor_of, own = 1.0, jax.random.fold_in(rng, 6)
    for position, parts in split:
        draws = jnp.exp(jax.random.uniform(jax.random.fold_in(own, position), (parts,), jnp.float32, least / len(split), high / len(split)))
        factor_of = factor_of * jnp.repeat(draws, shape[position] // parts).reshape([-1 if axis == position else 1 for axis in range(len(shape))])
    return factor_of


def normal_values(stream_key, extent, spread, most, cuts=(), dtype=jnp.bfloat16):
    values = jax.random.normal(stream_key, extent, jnp.float32) * spread
    if len(cuts) > 0:
        values = block_levels(stream_key, extent, cuts, -0.22, 0.18) * values
    return jnp.clip(values, min=-most, max=most).astype(dtype)


def gaussian_with(stream_key, shape, deviation, limit, shards, heavy, held_as=jnp.bfloat16):
    entries = deviation * jax.random.normal(stream_key, shape, jnp.float32)
    if shards:
        entries = entries * block_levels(stream_key, shape, shards, -0.22, 0.18)
    return jnp.clip(raised(entries, jax.random.fold_in(stream_key, 3), *heavy), -limit, limit).astype(held_as)


def setup_inputs(seed: int = 0) -> dict:
    key_list = jax.random.split(jax.random.key(seed), 5)
    return {
        "w_gate": gaussian_with(key_list[0], (EXPERTS, D_MODEL, D_EXPERT), D_MODEL ** -0.5, 0.25, ((0, 8), (1, 32)), (1, 2, 32, 2.75), jnp.float32),
        "w_up": gaussian_with(key_list[1], (EXPERTS, D_MODEL, D_EXPERT), D_MODEL ** -0.5, 0.25, ((0, 8), (1, 32)), (1, 2, 32, 2.75), jnp.float32),
        "router_weight": normal_values(key_list[2], (D_MODEL, EXPERTS), D_MODEL ** -0.5, 0.125, ((0, 32), (1, 8)), jnp.float32),
        "router_gain": jnp.clip(1.0 + 0.15 * jax.random.normal(key_list[3], (D_MODEL,), jnp.float32), 0.25, 1.75),
    }


def reference(w_gate, w_up, router_weight, router_gain):
    scale_gate = jnp.sum(jnp.abs(w_gate), axis=1) / D_MODEL
    serve_gate = (w_gate / jnp.expand_dims(scale_gate, 1)).astype(jnp.bfloat16)
    scale_up = jnp.sum(jnp.abs(w_up), axis=1) / D_MODEL
    serve_up = (w_up / jnp.expand_dims(scale_up, 1)).astype(jnp.bfloat16)
    serve_router = (router_weight * router_gain[:, None]).astype(jnp.bfloat16)
    return serve_gate, serve_up, scale_gate, scale_up, serve_router
```

```python
import functools

import jax
import jax.numpy as jnp
from jax import lax
from jax.experimental import pallas as pl
from jax.experimental.pallas import tpu as pltpu
from jax.sharding import PartitionSpec as P

D_MODEL = 2048
LANES = 128
HALF = LANES // 2
EXPERT_ROWS = 8


def sums_kernel(own, gate_ref, up_ref, router_ref, gain_ref, out_ref, gate_sums, up_sums):
    step = pl.program_id(0)
    gate_sums[pl.ds(step, 1), :] = jnp.sum(jnp.abs(gate_ref[0]), axis=0, keepdims=True)
    up_sums[pl.ds(step, 1), :] = jnp.sum(jnp.abs(up_ref[0]), axis=0, keepdims=True)

    @pl.when(step == pl.num_programs(0) - 1)
    def _():
        router = (router_ref[...] * gain_ref[...]).astype(jnp.bfloat16).astype(jnp.float32)
        router = jnp.concatenate([router, jnp.zeros_like(router)], axis=1)
        spare = jnp.zeros((EXPERT_ROWS, HALF - own), jnp.float32)
        for d in range(out_ref.shape[0]):
            columns = slice(d * own, (d + 1) * own)
            out_ref[d, 0] = jnp.concatenate(
                [gate_sums[:, columns], spare, up_sums[:, columns], spare], axis=1
            )
            out_ref[d, 1] = router


def column_sums(w_gate, w_up, router_weight, router_gain, size):
    experts, rows, width = w_gate.shape
    whole = lambda a: pl.BlockSpec(a.shape, lambda e: (0,) * a.ndim)
    router = router_weight.T
    gain = router_gain[None]
    expert = pl.BlockSpec((1, rows, width), lambda e: (e, 0, 0))
    shape = (size, 2, EXPERT_ROWS, LANES)
    return pl.pallas_call(
        functools.partial(sums_kernel, width // size),
        grid=(experts,),
        in_specs=[expert, expert, whole(router), whole(gain)],
        out_specs=pl.BlockSpec(shape, lambda e: (0, 0, 0, 0)),
        out_shape=jax.ShapeDtypeStruct(shape, jnp.float32),
        scratch_shapes=[pltpu.VMEM((experts, width), jnp.float32)] * 2,
        cost_estimate=pl.CostEstimate(flops=4_000_000, bytes_accessed=6_000_000, transcendentals=0),
        name="column_sums",
    )(w_gate, w_up, router, gain)


def turned_kernel(gate_ref, up_ref, out_ref):
    for e in range(gate_ref.shape[0]):
        both = jnp.concatenate([gate_ref[e], up_ref[e]], axis=0)
        out_ref[:, e, :] = both.T


def turned(w_gate, w_up):
    experts, rows, width = w_gate.shape
    block = pl.BlockSpec((experts, rows, LANES), lambda c: (0, 0, c))
    return pl.pallas_call(
        turned_kernel,
        grid=(width // LANES,),
        in_specs=[block, block],
        out_specs=pl.BlockSpec((LANES, experts, LANES), lambda c: (c, 0, 0)),
        out_shape=jax.ShapeDtypeStruct((width, experts, LANES), jnp.float32),
        cost_estimate=pl.CostEstimate(flops=8_000_000, bytes_accessed=12_000_000, transcendentals=0),
        name="turned",
    )(w_gate, w_up)


def scaled_kernel(own, turned_ref, scale_ref, out_ref):
    left = lax.broadcasted_iota(jnp.int32, (EXPERT_ROWS, LANES), 1) < HALF
    for d in range(scale_ref.shape[0]):
        inverse = 1.0 / scale_ref[d]
        for j in range(own):
            factor = jnp.where(left, inverse[:, j : j + 1], inverse[:, HALF + j : HALF + j + 1])
            out_ref[d, j] = (turned_ref[d * own + j] * factor).astype(jnp.bfloat16)


def scaled(tall, scales):
    width, experts, lanes = tall.shape
    size = scales.shape[0]
    own = width // size
    part = 4
    return pl.pallas_call(
        functools.partial(scaled_kernel, own),
        grid=(size // part,),
        in_specs=[
            pl.BlockSpec((part * own, experts, lanes), lambda c: (c, 0, 0)),
            pl.BlockSpec((part, EXPERT_ROWS, LANES), lambda c: (c, 0, 0)),
        ],
        out_specs=pl.BlockSpec((part, own, experts, lanes), lambda c: (c, 0, 0, 0)),
        out_shape=jax.ShapeDtypeStruct((size, own, experts, lanes), jnp.bfloat16),
        cost_estimate=pl.CostEstimate(flops=8_000_000, bytes_accessed=9_000_000, transcendentals=0),
        name="scaled",
    )(tall, scales)


def placed_kernel(arrived_ref, gate_ref, up_ref):
    for p in range(arrived_ref.shape[0] // 2):
        first, second = arrived_ref[2 * p], arrived_ref[2 * p + 1]
        lanes = slice(p * LANES, (p + 1) * LANES)
        gate_ref[:, :, lanes] = jnp.concatenate([first[..., :HALF], second[..., :HALF]], axis=-1)
        up_ref[:, :, lanes] = jnp.concatenate([first[..., HALF:], second[..., HALF:]], axis=-1)


def placed(arrived):
    size, own, experts, lanes = arrived.shape
    part = 11
    rows = size * HALF
    out = jax.ShapeDtypeStruct((own, experts, rows), jnp.bfloat16)
    return pl.pallas_call(
        placed_kernel,
        grid=(own // part,),
        in_specs=[pl.BlockSpec((size, part, experts, lanes), lambda c: (0, c, 0, 0))],
        out_specs=[pl.BlockSpec((part, experts, rows), lambda c: (c, 0, 0))] * 2,
        out_shape=[out, out],
        cost_estimate=pl.CostEstimate(flops=4_000_000, bytes_accessed=6_000_000, transcendentals=0),
        name="placed",
    )(arrived)


def exchanged(parts, axis):
    return lax.all_to_all(parts, axis, split_axis=0, concat_axis=0, tiled=True)


def on_device(w_gate, w_up, router_weight, router_gain):
    size = lax.axis_size("shard")
    own = w_gate.shape[2] // size
    sums = column_sums(w_gate, w_up, router_weight, router_gain, size)
    arrived = exchanged(sums, "shard")
    scale = jnp.sum(arrived[:, 0], axis=0) / D_MODEL
    scales = exchanged(jnp.broadcast_to(scale[None], (size, *scale.shape)), "shard")
    tall = turned(w_gate, w_up)
    serve = exchanged(scaled(tall, scales), "shard")
    serve_gate, serve_up = placed(serve)
    rows = arrived[:, 1, :, :HALF].astype(jnp.bfloat16)
    rows = jnp.transpose(rows, (1, 0, 2)).reshape(EXPERT_ROWS, -1)
    router = lax.all_gather(rows, "expert", axis=0, tiled=True)
    return (
        jnp.transpose(serve_gate, (1, 2, 0)),
        jnp.transpose(serve_up, (1, 2, 0)),
        scale[:, :own],
        scale[:, HALF : HALF + own],
        router.T,
    )


def solution(mesh):
    placed_in = (
        P("expert", "shard", None),
        P("expert", "shard", None),
        P("shard", "expert"),
        P("shard"),
    )
    return jax.shard_map(
        on_device,
        mesh=mesh,
        in_specs=placed_in,
        out_specs=(
            P("expert", None, "shard"),
            P("expert", None, "shard"),
            P("expert", "shard"),
            P("expert", "shard"),
            P(),
        ),
        check_vma=False,
    )
```

```python
import jax
import jax.numpy as jnp
from jax import lax
from jax.experimental import pallas as pl
from jax.experimental.pallas import tpu as pltpu
from jax.sharding import PartitionSpec as P

D_MODEL = 2048
LANES = 128
HALF = LANES // 2
IN_HBM = pl.BlockSpec(memory_space=pltpu.HBM)
IN_VMEM = pl.BlockSpec(memory_space=pltpu.VMEM)


def in_hbm(x):
    return pltpu.with_memory_space_constraint(x, pltpu.HBM)


def in_vmem(x):
    return pltpu.with_memory_space_constraint(x, pltpu.VMEM)


def sums_kernel(
    gate, up, router, gain, out, gate_held, up_held,
    router_held, gain_held, sums, w_sems, small_sems, out_sem,
):
    experts = gate.shape[0]
    size = out.shape[0]
    own = gate.shape[2] // size
    small = [
        pltpu.make_async_copy(router, router_held, small_sems.at[0]),
        pltpu.make_async_copy(gain, gain_held, small_sems.at[1]),
    ]
    for copy in small:
        copy.start()
    pairs = [
        (
            pltpu.make_async_copy(gate.at[e], gate_held.at[e], w_sems.at[e, 0]),
            pltpu.make_async_copy(up.at[e], up_held.at[e], w_sems.at[e, 1]),
        )
        for e in range(experts)
    ]
    for pair in pairs:
        for copy in pair:
            copy.start()
    for copy in small:
        copy.wait()
    part = (router_held[...] * gain_held[...]).astype(jnp.bfloat16).astype(jnp.float32)
    part = jnp.concatenate([part, jnp.zeros_like(part)], axis=1)
    for d in range(size):
        sums[d, 1] = part
    gate_sums, up_sums = [], []
    for e in range(experts):
        pairs[e][0].wait()
        gate_sums.append(jnp.sum(jnp.abs(gate_held[e]), axis=0, keepdims=True))
        pairs[e][1].wait()
        up_sums.append(jnp.sum(jnp.abs(up_held[e]), axis=0, keepdims=True))
    gate_sums = jnp.concatenate(gate_sums, axis=0)
    up_sums = jnp.concatenate(up_sums, axis=0)
    spare = jnp.zeros((experts, HALF - own), jnp.float32)
    for d in range(size):
        columns = slice(d * own, (d + 1) * own)
        sums[d, 0] = jnp.concatenate(
            [gate_sums[:, columns], spare, up_sums[:, columns], spare], axis=1
        )
    copy = pltpu.make_async_copy(sums, out, out_sem)
    copy.start()
    copy.wait()


def column_sums(w_gate, w_up, router_weight, router_gain, size):
    experts = w_gate.shape[0]
    router, gain = router_weight.T, router_gain[None]
    shape = (size, 2, experts, LANES)
    return pl.pallas_call(
        sums_kernel,
        in_specs=[IN_HBM] * 4,
        out_specs=[IN_HBM, IN_VMEM, IN_VMEM],
        out_shape=[
            jax.ShapeDtypeStruct(shape, jnp.float32),
            pltpu.VMEM(w_gate.shape, jnp.float32),
            pltpu.VMEM(w_up.shape, jnp.float32),
        ],
        scratch_shapes=[
            pltpu.VMEM(router.shape, jnp.float32),
            pltpu.VMEM(gain.shape, jnp.float32),
            pltpu.VMEM(shape, jnp.float32),
            pltpu.SemaphoreType.DMA((experts, 2)),
            pltpu.SemaphoreType.DMA((2,)),
            pltpu.SemaphoreType.DMA,
        ],
        compiler_params=pltpu.CompilerParams(vmem_limit_bytes=8 << 20),
        cost_estimate=pl.CostEstimate(flops=4_000_000, bytes_accessed=6_000_000, transcendentals=0),
        name="column_sums",
    )(in_hbm(w_gate), in_hbm(w_up), in_hbm(router), in_hbm(gain))


def packed_kernel(gate, up, scales, out, held, sems):
    experts, _, width = gate.shape
    size = scales.shape[0]
    own = width // size
    gate_inverse = 1.0 / jnp.concatenate([scales[d, :, :own] for d in range(size)], axis=1)
    up_inverse = 1.0 / jnp.concatenate([scales[d, :, HALF : HALF + own] for d in range(size)], axis=1)
    copies = []
    for c in range(width // LANES):
        columns = slice(c * LANES, (c + 1) * LANES)
        turned = []
        for e in range(experts):
            both = jnp.concatenate(
                [
                    gate[e, :, columns] * gate_inverse[e : e + 1, columns],
                    up[e, :, columns] * up_inverse[e : e + 1, columns],
                ],
                axis=0,
            )
            turned.append(both.astype(jnp.bfloat16).T)
        held[columns] = jnp.swapaxes(jnp.stack(turned), 0, 1)
        rows = pl.ds(c * LANES, LANES)
        copies.append(pltpu.make_async_copy(held.at[rows], out.at[rows], sems.at[c]))
        copies[-1].start()
    for copy in copies:
        copy.wait()


def packed(w_gate, w_up, scales):
    experts, rows, width = w_gate.shape
    size = scales.shape[0]
    shape = (width, experts, 2 * rows)
    out = pl.pallas_call(
        packed_kernel,
        in_specs=[IN_VMEM] * 3,
        out_specs=IN_HBM,
        out_shape=pltpu.HBM(shape, jnp.bfloat16),
        scratch_shapes=[
            pltpu.VMEM(shape, jnp.bfloat16),
            pltpu.SemaphoreType.DMA((width // LANES,)),
        ],
        compiler_params=pltpu.CompilerParams(vmem_limit_bytes=12 << 20),
        cost_estimate=pl.CostEstimate(flops=8_000_000, bytes_accessed=9_000_000, transcendentals=0),
        name="packed",
    )(in_vmem(w_gate), in_vmem(w_up), in_vmem(scales))
    return out.reshape(size, width // size, experts, 2 * rows)


def placed_kernel(arrived, gate, up, gate_held, up_held, sems):
    size, total, _ = arrived.shape
    pieces = sems.shape[0]
    step = total // pieces
    copies = []
    for c in range(pieces):
        rows = slice(c * step, (c + 1) * step)
        for p in range(size // 2):
            first, second = arrived[2 * p, rows], arrived[2 * p + 1, rows]
            lanes = slice(p * LANES, (p + 1) * LANES)
            gate_held[rows, lanes] = jnp.concatenate([first[:, :HALF], second[:, :HALF]], axis=-1)
            up_held[rows, lanes] = jnp.concatenate([first[:, HALF:], second[:, HALF:]], axis=-1)
        part = pl.ds(c * step, step)
        for t, (held, out) in enumerate(((gate_held, gate), (up_held, up))):
            copies.append(pltpu.make_async_copy(held.at[part], out.at[part], sems.at[c, t]))
            copies[-1].start()
    for copy in copies:
        copy.wait()


def placed(arrived):
    size, own, experts, lanes = arrived.shape
    pieces = 11
    shape = (own * experts, size * HALF)
    out = jax.ShapeDtypeStruct(shape, jnp.bfloat16)
    results = pl.pallas_call(
        placed_kernel,
        in_specs=[IN_VMEM],
        out_specs=[IN_HBM] * 2,
        out_shape=[out, out],
        scratch_shapes=[
            pltpu.VMEM(shape, jnp.bfloat16),
            pltpu.VMEM(shape, jnp.bfloat16),
            pltpu.SemaphoreType.DMA((pieces, 2)),
        ],
        compiler_params=pltpu.CompilerParams(vmem_limit_bytes=12 << 20),
        cost_estimate=pl.CostEstimate(flops=4_000_000, bytes_accessed=6_000_000, transcendentals=0),
        name="placed",
    )(in_vmem(arrived.reshape(size, own * experts, lanes)))
    return [r.reshape(own, experts, size * HALF) for r in results]


def stored_kernel(held, out, sem):
    copy = pltpu.make_async_copy(held, out, sem)
    copy.start()
    copy.wait()


def stored(x):
    return pl.pallas_call(
        stored_kernel,
        in_specs=[IN_VMEM],
        out_specs=IN_HBM,
        out_shape=jax.ShapeDtypeStruct(x.shape, x.dtype),
        scratch_shapes=[pltpu.SemaphoreType.DMA],
        compiler_params=pltpu.CompilerParams(vmem_limit_bytes=1 << 20),
        cost_estimate=pl.CostEstimate(flops=1_000_000, bytes_accessed=500_000, transcendentals=0),
        name="stored",
    )(in_vmem(x))


def exchanged(parts, axis):
    return lax.all_to_all(parts, axis, split_axis=0, concat_axis=0, tiled=True)


def on_device(w_gate, w_up, router_weight, router_gain):
    size = lax.axis_size("shard")
    experts, _, width = w_gate.shape
    own = width // size
    sums, w_gate, w_up = column_sums(w_gate, w_up, router_weight, router_gain, size)
    arrived = exchanged(sums, "shard")
    scale = jnp.sum(arrived[:, 0], axis=0) / D_MODEL
    scales = exchanged(jnp.broadcast_to(scale[None], (size, *scale.shape)), "shard")
    serve = exchanged(packed(w_gate, w_up, scales), "shard")
    serve_gate, serve_up = placed(serve)
    rows = arrived[:, 1, :, :HALF].astype(jnp.bfloat16)
    rows = jnp.transpose(rows, (1, 0, 2)).reshape(experts, -1)
    router = lax.all_gather(rows, "expert", axis=0, tiled=True)
    return (
        jnp.transpose(serve_gate, (1, 2, 0)),
        jnp.transpose(serve_up, (1, 2, 0)),
        scale[:, :own],
        scale[:, HALF : HALF + own],
        stored(router).T,
    )


def solution(mesh):
    return jax.shard_map(
        on_device,
        mesh=mesh,
        in_specs=(
            P("expert", "shard", None),
            P("expert", "shard", None),
            P("shard", "expert"),
            P("shard"),
        ),
        out_specs=(
            P("expert", None, "shard"),
            P("expert", None, "shard"),
            P("expert", "shard"),
            P("expert", "shard"),
            P(),
        ),
        check_vma=False,
    )
```

```python
import functools

import jax
import jax.numpy as jnp
from jax import lax
from jax.experimental import pallas as pl
from jax.experimental.pallas import tpu as pltpu
from jax.sharding import PartitionSpec as P


D_MODEL = 2048
LANES = 128
HALF = LANES // 2
Z, Y = 8, 4
ALONG_Y = [[z * Y + y for y in range(Y)] for z in range(Z)]
ALONG_Z = [[z * Y + y for z in range(Z)] for y in range(Y)]
SHIFTS = (0, 1, 7, 4, 3, 5, 2, 6)
RAW = 8
PIECE = 80
HEAD = 6 * LANES
IN_HBM = pl.BlockSpec(memory_space=pltpu.HBM)
IN_VMEM = pl.BlockSpec(memory_space=pltpu.VMEM)


def in_hbm(x):
    return pltpu.with_memory_space_constraint(x, pltpu.HBM)


def in_vmem(x):
    return pltpu.with_memory_space_constraint(x, pltpu.VMEM)


def opened_kernel(gate, up, router, gain, *refs):
    out, gate_head, up_head, *blocks = refs[: 3 + Z]
    (
        gate_tail, up_tail, router_held, gain_held, sums, held, w_sems, small_sems, sums_sem, block_sems,
    ) = refs[3 + Z :]
    experts, _, width = gate.shape
    own = width // (Y * Z)
    loads = [
        [
            (
                pltpu.make_async_copy(w.at[e, :, pl.ds(0, HEAD)], head.at[e], w_sems.at[e, t, 0]),
                pltpu.make_async_copy(
                    w.at[e, :, pl.ds(HEAD, width - HEAD)], tail.at[e], w_sems.at[e, t, 1]
                ),
            )
            for t, (w, head, tail) in enumerate(((gate, gate_head, gate_tail), (up, up_head, up_tail)))
        ]
        for e in range(experts)
    ]
    small = [
        pltpu.make_async_copy(router, router_held, small_sems.at[0]),
        pltpu.make_async_copy(gain, gain_held, small_sems.at[1]),
    ]
    for pairs in loads:
        for pair in pairs:
            for copy in pair:
                copy.start()
    for copy in small:
        copy.start()
    rows = ([], [])
    for e in range(experts):
        for t, (head, tail) in enumerate(((gate_head, gate_tail), (up_head, up_tail))):
            totals = []
            for part, copy in zip((head, tail), loads[e][t]):
                copy.wait()
                totals.append(jnp.sum(jnp.abs(part[e]), axis=0, keepdims=True))
            rows[t].append(jnp.concatenate(totals, axis=1))
    gate_sums, up_sums = (jnp.concatenate(r, axis=0) for r in rows)
    spare = jnp.zeros((experts, HALF - own), jnp.float32)
    for d in range(Y * Z):
        mine = slice(d * own, (d + 1) * own)
        sums[d % Y, d // Y] = jnp.concatenate([gate_sums[:, mine], spare, up_sums[:, mine], spare], axis=1)
    copies = [pltpu.make_async_copy(sums, out, sums_sem)]
    copies[0].start()
    for copy in small:
        copy.wait()
    part = (router_held[...] * gain_held[...]).astype(jnp.bfloat16).astype(jnp.float32)
    part = jnp.concatenate([part, jnp.zeros_like(part)], axis=1)
    for z in range(Z):
        held[z, Y * RAW] = part
    for c in range(width // LANES):
        if c * LANES < HEAD:
            sources, first = (gate_head, up_head), c * LANES
        else:
            sources, first = (gate_tail, up_tail), c * LANES - HEAD
        columns = slice(first, first + LANES)
        turned = [jnp.concatenate([w[e, :, columns] for w in sources], axis=0).T for e in range(experts)]
        for d in range(Y * Z):
            low = max(d * own, c * LANES)
            high = min(d * own + RAW, (c + 1) * LANES)
            if low < high:
                part = jnp.stack([t[low - c * LANES : high - c * LANES] for t in turned])
                place = slice(d % Y * RAW + low - d * own, d % Y * RAW + high - d * own)
                held[d // Y, place] = jnp.swapaxes(part, 0, 1)
    z = lax.axis_index("shard") // Y
    for k, shift in enumerate(SHIFTS):
        copies.append(pltpu.make_async_copy(held.at[lax.rem(z + shift, Z)], blocks[k], block_sems.at[k]))
        copies[-1].start()
    for copy in copies:
        copy.wait()


def opened(w_gate, w_up, router_weight, router_gain):
    experts, rows, width = w_gate.shape
    router, gain = router_weight.T, router_gain[None]
    shape = (Y, Z, experts, LANES)
    block = (Y * RAW + 1, experts, LANES)
    head = pltpu.VMEM((experts, rows, HEAD), jnp.float32)
    tail = pltpu.VMEM((experts, rows, width - HEAD), jnp.float32)
    out, gate_head, up_head, *blocks = pl.pallas_call(
        opened_kernel,
        in_specs=[IN_HBM] * 4,
        out_specs=[IN_HBM, IN_VMEM, IN_VMEM] + [IN_HBM] * Z,
        out_shape=[pltpu.HBM(shape, jnp.float32), head, head] + [pltpu.HBM(block, jnp.float32)] * Z,
        scratch_shapes=[
            tail,
            tail,
            pltpu.VMEM(router.shape, jnp.float32),
            pltpu.VMEM(gain.shape, jnp.float32),
            pltpu.VMEM(shape, jnp.float32),
            pltpu.VMEM((Z, *block), jnp.float32),
            pltpu.SemaphoreType.DMA((experts, 2, 2)),
            pltpu.SemaphoreType.DMA((2,)),
            pltpu.SemaphoreType.DMA,
            pltpu.SemaphoreType.DMA((Z,)),
        ],
        compiler_params=pltpu.CompilerParams(vmem_limit_bytes=10 << 20),
        cost_estimate=pl.CostEstimate(flops=8_000_000, bytes_accessed=8_000_000, transcendentals=0),
        name="opened",
    )(in_hbm(w_gate), in_hbm(w_up), in_hbm(router), in_hbm(gain))
    return out, (gate_head, up_head), blocks


def regrouped_kernel(*refs):
    blocks, outs, pieces = refs[:Z], refs[Z : Z + Y], refs[Z + Y]
    held, in_sems, out_sems, piece_sem = refs[Z + Y + 1 :]
    y = lax.rem(lax.axis_index("shard"), Y)
    copies = [pltpu.make_async_copy(blocks[k], held.at[k], in_sems.at[k]) for k in range(Z)]
    for copy in copies:
        copy.start()
    for copy in copies:
        copy.wait()
    copies = [pltpu.make_async_copy(held.at[:, Y * RAW], pieces, piece_sem)] + [
        pltpu.make_async_copy(
            held.at[:, pl.ds(lax.rem(y + t, Y) * RAW, RAW)], outs[t], out_sems.at[t]
        )
        for t in range(Y)
    ]
    for copy in copies:
        copy.start()
    for copy in copies:
        copy.wait()


def regrouped(blocks):
    rest = blocks[0].shape[1:]
    return pl.pallas_call(
        regrouped_kernel,
        in_specs=[IN_HBM] * Z,
        out_specs=[IN_HBM] * (Y + 1),
        out_shape=[pltpu.HBM((Z, RAW, *rest), jnp.float32)] * Y + [pltpu.HBM((Z, *rest), jnp.float32)],
        scratch_shapes=[
            pltpu.VMEM((Z, *blocks[0].shape), jnp.float32),
            pltpu.SemaphoreType.DMA((Z,)),
            pltpu.SemaphoreType.DMA((Y,)),
            pltpu.SemaphoreType.DMA,
        ],
        compiler_params=pltpu.CompilerParams(vmem_limit_bytes=3 << 20),
        cost_estimate=pl.CostEstimate(flops=8_000_000, bytes_accessed=2_000_000, transcendentals=0),
        name="regrouped",
    )(*[in_hbm(b) for b in blocks])


def in_source_order(blocks, held, sems):
    me = lax.axis_index("shard")
    z, y = me // Y, lax.rem(me, Y)
    copies = []
    for t in range(Y):
        for k, shift in enumerate(SHIFTS):
            source = lax.rem(z + Z - shift, Z) * Y + lax.rem(y + Y - t, Y)
            copies.append(pltpu.make_async_copy(blocks[t].at[k], held.at[source], sems.at[t, k]))
    return copies


def rows_kernel(*refs):
    blocks, router, (held, sems) = refs[:Y], refs[Y], refs[Y + 1 :]
    copies = in_source_order(blocks, held, sems)
    for copy in copies:
        copy.start()
    for copy in copies:
        copy.wait()
    for p in range(Y * Z // 2):
        both = jnp.concatenate([held[2 * p][:, :HALF], held[2 * p + 1][:, :HALF]], axis=1)
        router[:, p * LANES : (p + 1) * LANES] = both.astype(jnp.bfloat16)


def router_rows(pieces):
    experts = pieces[0].shape[1]
    return pl.pallas_call(
        rows_kernel,
        in_specs=[IN_HBM] * Y,
        out_specs=IN_VMEM,
        out_shape=pltpu.VMEM((experts, Y * Z * HALF), jnp.bfloat16),
        scratch_shapes=[
            pltpu.VMEM((Y * Z, *pieces[0].shape[1:]), jnp.float32),
            pltpu.SemaphoreType.DMA((Y, Z)),
        ],
        compiler_params=pltpu.CompilerParams(vmem_limit_bytes=1 << 20),
        cost_estimate=pl.CostEstimate(flops=1_000_000, bytes_accessed=300_000, transcendentals=0),
        name="router_rows",
    )(*[in_hbm(b) for b in pieces])


def finished_kernel(*refs):
    blocks, scale, (gate, up), (held, sems) = refs[:Y], refs[Y], refs[Y + 1 : Y + 3], refs[Y + 3 :]
    copies = in_source_order(blocks, held, sems)
    for copy in copies:
        copy.start()
    inverse = 1.0 / scale[...]
    rows = inverse.shape[0]
    for copy in copies:
        copy.wait()
    for p in range(Y * Z // 2):
        lanes = slice(p * LANES, (p + 1) * LANES)
        for j in range(RAW):
            first, second = held[2 * p, j], held[2 * p + 1, j]
            place = slice(j * rows, (j + 1) * rows)
            for out, low in ((gate, 0), (up, HALF)):
                factor = jnp.broadcast_to(inverse[:, low + j : low + j + 1], (rows, LANES))
                both = jnp.concatenate([first[:, low : low + HALF], second[:, low : low + HALF]], axis=1)
                out[place, lanes] = (both * factor).astype(jnp.bfloat16)


def finished(blocks, scale):
    experts = scale.shape[0]
    out = pltpu.VMEM((RAW * experts, Y * Z * HALF), jnp.bfloat16)
    return pl.pallas_call(
        finished_kernel,
        in_specs=[IN_HBM] * Y + [IN_VMEM],
        out_specs=[IN_VMEM] * 2,
        out_shape=[out, out],
        scratch_shapes=[
            pltpu.VMEM((Y * Z, *blocks[0].shape[1:]), jnp.float32),
            pltpu.SemaphoreType.DMA((Y, Z)),
        ],
        compiler_params=pltpu.CompilerParams(vmem_limit_bytes=6 << 20),
        cost_estimate=pl.CostEstimate(flops=8_000_000, bytes_accessed=3_000_000, transcendentals=0),
        name="finished",
    )(*[in_hbm(b) for b in blocks], in_vmem(scale))


def packed_kernel(gate, up, gate_head, up_head, scales, out, tails, held, tail_sems, sems):
    experts, _, width = gate.shape
    size = Y * Z
    loads = [
        [
            pltpu.make_async_copy(w.at[:, :, pl.ds(low, LANES)], tails.at[c, t], tail_sems.at[c, t])
            for t, w in enumerate((gate, up))
        ]
        for c, low in enumerate(range(HEAD, width, LANES))
    ]
    for pair in loads:
        for copy in pair:
            copy.start()
    own = width // size
    tiles = [scales[d % Y, d // Y] for d in range(size)]
    gate_inverse = 1.0 / jnp.concatenate([t[:, :own] for t in tiles], axis=1)
    up_inverse = 1.0 / jnp.concatenate([t[:, HALF : HALF + own] for t in tiles], axis=1)
    copies = []
    for c in range(width // LANES):
        columns = slice(c * LANES, (c + 1) * LANES)
        tail = c - HEAD // LANES
        if tail >= 0:
            for copy in loads[tail]:
                copy.wait()
        turned = []
        for e in range(experts):
            if tail < 0:
                parts = gate_head[e, :, columns], up_head[e, :, columns]
            else:
                parts = tails[tail, 0, e], tails[tail, 1, e]
            both = jnp.concatenate(
                [
                    parts[0] * gate_inverse[e : e + 1, columns],
                    parts[1] * up_inverse[e : e + 1, columns],
                ],
                axis=0,
            )
            turned.append(both.astype(jnp.bfloat16).T)
        held[columns] = jnp.swapaxes(jnp.stack(turned), 0, 1)
        while len(copies) < size and (len(copies) + 1) * own <= (c + 1) * LANES:
            d = len(copies)
            rows = pl.ds(d * own + RAW, own - RAW)
            copies.append(pltpu.make_async_copy(held.at[rows], out.at[d], sems.at[d]))
            copies[-1].start()
    for copy in copies:
        copy.wait()


def packed(w_gate, w_up, gate_head, up_head, scales):
    experts, rows, width = w_gate.shape
    size = Y * Z
    return pl.pallas_call(
        packed_kernel,
        in_specs=[IN_HBM] * 2 + [IN_VMEM] * 3,
        out_specs=IN_HBM,
        out_shape=pltpu.HBM((size, width // size - RAW, experts, 2 * rows), jnp.bfloat16),
        scratch_shapes=[
            pltpu.VMEM(((width - HEAD) // LANES, 2, experts, rows, LANES), jnp.float32),
            pltpu.VMEM((width, experts, 2 * rows), jnp.bfloat16),
            pltpu.SemaphoreType.DMA(((width - HEAD) // LANES, 2)),
            pltpu.SemaphoreType.DMA((size,)),
        ],
        compiler_params=pltpu.CompilerParams(vmem_limit_bytes=12 << 20),
        cost_estimate=pl.CostEstimate(flops=8_000_000, bytes_accessed=9_000_000, transcendentals=0),
        name="packed",
    )(in_hbm(w_gate), in_hbm(w_up), in_vmem(gate_head), in_vmem(up_head), in_vmem(scales))


def placed_kernel(arrived, raw_gate, raw_up, gate, up, gate_held, up_held, raw_sems, sems):
    size, total, _ = arrived.shape
    raw = raw_gate.shape[0]
    copies = []
    for t, (part, out) in enumerate(((raw_gate, gate), (raw_up, up))):
        copies.append(pltpu.make_async_copy(part, out.at[pl.ds(0, raw)], raw_sems.at[t]))
        copies[-1].start()
    for c, low in enumerate(range(0, total, PIECE)):
        high = min(low + PIECE, total)
        rows = slice(low, high)
        for p in range(size // 2):
            first, second = arrived[2 * p, rows], arrived[2 * p + 1, rows]
            lanes = slice(p * LANES, (p + 1) * LANES)
            gate_held[rows, lanes] = jnp.concatenate([first[:, :HALF], second[:, :HALF]], axis=-1)
            up_held[rows, lanes] = jnp.concatenate([first[:, HALF:], second[:, HALF:]], axis=-1)
        for t, (held, out) in enumerate(((gate_held, gate), (up_held, up))):
            copies.append(
                pltpu.make_async_copy(
                    held.at[pl.ds(low, high - low)],
                    out.at[pl.ds(raw + low, high - low)],
                    sems.at[c, t],
                )
            )
            copies[-1].start()
    for copy in copies:
        copy.wait()


def placed(arrived, raw_gate, raw_up):
    size, rest, experts, lanes = arrived.shape
    held = (rest * experts, size * HALF)
    shape = ((rest + RAW) * experts, size * HALF)
    out = jax.ShapeDtypeStruct(shape, jnp.bfloat16)
    results = pl.pallas_call(
        placed_kernel,
        in_specs=[IN_VMEM] * 3,
        out_specs=[IN_HBM] * 2,
        out_shape=[out, out],
        scratch_shapes=[
            pltpu.VMEM(held, jnp.bfloat16),
            pltpu.VMEM(held, jnp.bfloat16),
            pltpu.SemaphoreType.DMA((2,)),
            pltpu.SemaphoreType.DMA((pl.cdiv(held[0], PIECE), 2)),
        ],
        compiler_params=pltpu.CompilerParams(vmem_limit_bytes=12 << 20),
        cost_estimate=pl.CostEstimate(flops=4_000_000, bytes_accessed=6_000_000, transcendentals=0),
        name="placed",
    )(in_vmem(arrived.reshape(size, rest * experts, lanes)), in_vmem(raw_gate), in_vmem(raw_up))
    return [r.reshape(rest + RAW, experts, size * HALF) for r in results]


def stored_kernel(held, out, sem):
    copy = pltpu.make_async_copy(held, out, sem)
    copy.start()
    copy.wait()


def stored(x):
    return pl.pallas_call(
        stored_kernel,
        in_specs=[IN_VMEM],
        out_specs=IN_HBM,
        out_shape=jax.ShapeDtypeStruct(x.shape, x.dtype),
        scratch_shapes=[pltpu.SemaphoreType.DMA],
        compiler_params=pltpu.CompilerParams(vmem_limit_bytes=1 << 20),
        cost_estimate=pl.CostEstimate(flops=1_000_000, bytes_accessed=500_000, transcendentals=0),
        name="stored",
    )(in_vmem(x))


def summed_kernel(share, arrived, out, *refs):
    *mine, held, sems = refs
    held[...] = jnp.sum(arrived[...], axis=0) * share
    copies = [pltpu.make_async_copy(held, out.at[i], sems.at[i]) for i in range(out.shape[0])]
    for copy in copies:
        copy.start()
    for ref in mine:
        ref[...] = held[lax.axis_index("shard") // Y]
    for copy in copies:
        copy.wait()


def summed(arrived, count, share, mine=False):
    shape = arrived.shape[1:]
    return pl.pallas_call(
        functools.partial(summed_kernel, share),
        in_specs=[IN_VMEM],
        out_specs=[IN_HBM, IN_VMEM][: 1 + mine],
        out_shape=[
            pltpu.HBM((count, *shape), jnp.float32),
            pltpu.VMEM(shape[1:], jnp.float32),
        ][: 1 + mine],
        scratch_shapes=[pltpu.VMEM(shape, jnp.float32), pltpu.SemaphoreType.DMA((count,))],
        compiler_params=pltpu.CompilerParams(vmem_limit_bytes=1 << 20),
        cost_estimate=pl.CostEstimate(flops=1_000_000, bytes_accessed=500_000, transcendentals=0),
        name="summed",
    )(in_vmem(arrived))


def exchanged(parts, groups=None):
    return lax.all_to_all(
        parts, "shard", split_axis=0, concat_axis=0, tiled=True, axis_index_groups=groups
    )


def shifted(x, z_shift, y_shift):
    pairs = [
        (z * Y + y, (z + z_shift) % Z * Y + (y + y_shift) % Y) for z in range(Z) for y in range(Y)
    ]
    return lax.ppermute(x, "shard", pairs)


def on_device(w_gate, w_up, router_weight, router_gain):
    own = w_gate.shape[2] // (Y * Z)
    sums, heads, blocks = opened(w_gate, w_up, router_weight, router_gain)
    sums = exchanged(sums, ALONG_Y)
    (sums,) = summed(sums, Z, 1.0)
    sums = exchanged(sums, ALONG_Z)
    moved = [blocks[0]]
    for k, shift in enumerate(SHIFTS):
        if k:
            moved.append(shifted(blocks[k], shift, 0))
    scales, scale = summed(sums, Y, 1.0 / D_MODEL, mine=True)
    scales = exchanged(scales, ALONG_Y)
    serve = packed(w_gate, w_up, *heads, scales)
    serve = exchanged(serve)
    *moved, pieces = regrouped(moved)
    pieces = [pieces]
    for t in range(1, Y):
        pieces.append(shifted(pieces[0], 0, t))
    for t in range(1, Y):
        moved[t] = shifted(moved[t], 0, t)
    rows = router_rows(pieces)
    router = lax.all_gather(rows, "expert", axis=0, tiled=True)
    router = stored(router)
    raw_gate, raw_up = finished(moved, scale)
    serve_gate, serve_up = placed(serve, raw_gate, raw_up)
    return (
        jnp.transpose(serve_gate, (1, 2, 0)),
        jnp.transpose(serve_up, (1, 2, 0)),
        scale[:, :own],
        scale[:, HALF : HALF + own],
        router.T,
    )


def solution(mesh):
    return jax.shard_map(
        on_device,
        mesh=mesh,
        in_specs=(
            P("expert", "shard", None),
            P("expert", "shard", None),
            P("shard", "expert"),
            P("shard"),
        ),
        out_specs=(
            P("expert", None, "shard"),
            P("expert", None, "shard"),
            P("expert", "shard"),
            P("expert", "shard"),
            P(),
        ),
        check_vma=False,
    )
```

```python
import functools

import jax
import jax.numpy as jnp
from jax import lax
from jax.experimental import pallas as pl
from jax.experimental.pallas import tpu as pltpu
from jax.sharding import PartitionSpec as P


D_MODEL = 2048
LANES = 128
HALF = LANES // 2
Z, Y = 8, 4
ALONG_Y = [[z * Y + y for y in range(Y)] for z in range(Z)]
ALONG_Z = [[z * Y + y for z in range(Z)] for y in range(Y)]
SHIFTS = (0, 1, 7, 4, 3, 5, 2, 6)
RAW = 8
PIECE = 80
HEAD = 6 * LANES
IN_HBM = pl.BlockSpec(memory_space=pltpu.HBM)
IN_VMEM = pl.BlockSpec(memory_space=pltpu.VMEM)


def in_hbm(x):
    return pltpu.with_memory_space_constraint(x, pltpu.HBM)


def in_vmem(x):
    return pltpu.with_memory_space_constraint(x, pltpu.VMEM)


def opened_kernel(gate, up, router, gain, *refs):
    out, gate_head, up_head, *blocks = refs[: 3 + Z]
    (
        gate_tail, up_tail, router_held, gain_held, sums, held, w_sems, small_sems, sums_sem, block_sems,
    ) = refs[3 + Z :]
    experts, _, width = gate.shape
    own = width // (Y * Z)
    loads = [
        [
            (
                pltpu.make_async_copy(w.at[e, :, pl.ds(0, HEAD)], head.at[e], w_sems.at[e, t, 0]),
                pltpu.make_async_copy(
                    w.at[e, :, pl.ds(HEAD, width - HEAD)], tail.at[e], w_sems.at[e, t, 1]
                ),
            )
            for t, (w, head, tail) in enumerate(((gate, gate_head, gate_tail), (up, up_head, up_tail)))
        ]
        for e in range(experts)
    ]
    small = [
        pltpu.make_async_copy(router, router_held, small_sems.at[0]),
        pltpu.make_async_copy(gain, gain_held, small_sems.at[1]),
    ]
    for pairs in loads:
        for pair in pairs:
            for copy in pair:
                copy.start()
    for copy in small:
        copy.start()
    rows = ([], [])
    for e in range(experts):
        for t, (head, tail) in enumerate(((gate_head, gate_tail), (up_head, up_tail))):
            totals = []
            for part, copy in zip((head, tail), loads[e][t]):
                copy.wait()
                totals.append(jnp.sum(jnp.abs(part[e]), axis=0, keepdims=True))
            rows[t].append(jnp.concatenate(totals, axis=1))
    gate_sums, up_sums = (jnp.concatenate(r, axis=0) for r in rows)
    spare = [jnp.ones((experts, sums.shape[2] - 2 * own * Z), jnp.float32)]
    for y in range(Y):
        parts = []
        for z in range(Z):
            mine = slice((z * Y + y) * own, (z * Y + y + 1) * own)
            parts += [gate_sums[:, mine], up_sums[:, mine]]
        sums[y] = jnp.concatenate(parts + spare, axis=1)
    copies = [pltpu.make_async_copy(sums, out, sums_sem)]
    copies[0].start()
    for copy in small:
        copy.wait()
    part = (router_held[...] * gain_held[...]).astype(jnp.bfloat16).astype(jnp.float32)
    part = jnp.concatenate([part, jnp.zeros_like(part)], axis=1)
    for z in range(Z):
        held[z, Y * RAW] = part
    for c in range(width // LANES):
        if c * LANES < HEAD:
            sources, first = (gate_head, up_head), c * LANES
        else:
            sources, first = (gate_tail, up_tail), c * LANES - HEAD
        columns = slice(first, first + LANES)
        turned = [jnp.concatenate([w[e, :, columns] for w in sources], axis=0).T for e in range(experts)]
        for d in range(Y * Z):
            low = max(d * own, c * LANES)
            high = min(d * own + RAW, (c + 1) * LANES)
            if low < high:
                part = jnp.stack([t[low - c * LANES : high - c * LANES] for t in turned])
                place = slice(d % Y * RAW + low - d * own, d % Y * RAW + high - d * own)
                held[d // Y, place] = jnp.swapaxes(part, 0, 1)
    z = lax.axis_index("shard") // Y
    for k, shift in enumerate(SHIFTS):
        copies.append(pltpu.make_async_copy(held.at[lax.rem(z + shift, Z)], blocks[k], block_sems.at[k]))
        copies[-1].start()
    for copy in copies:
        copy.wait()


def opened(w_gate, w_up, router_weight, router_gain):
    experts, rows, width = w_gate.shape
    router, gain = router_weight.T, router_gain[None]
    shape = (Y, experts, pl.cdiv(2 * width // Y, LANES) * LANES)
    block = (Y * RAW + 1, experts, LANES)
    head = pltpu.VMEM((experts, rows, HEAD), jnp.float32)
    tail = pltpu.VMEM((experts, rows, width - HEAD), jnp.float32)
    out, gate_head, up_head, *blocks = pl.pallas_call(
        opened_kernel,
        in_specs=[IN_HBM] * 4,
        out_specs=[IN_HBM, IN_VMEM, IN_VMEM] + [IN_HBM] * Z,
        out_shape=[pltpu.HBM(shape, jnp.float32), head, head] + [pltpu.HBM(block, jnp.float32)] * Z,
        scratch_shapes=[
            tail,
            tail,
            pltpu.VMEM(router.shape, jnp.float32),
            pltpu.VMEM(gain.shape, jnp.float32),
            pltpu.VMEM(shape, jnp.float32),
            pltpu.VMEM((Z, *block), jnp.float32),
            pltpu.SemaphoreType.DMA((experts, 2, 2)),
            pltpu.SemaphoreType.DMA((2,)),
            pltpu.SemaphoreType.DMA,
            pltpu.SemaphoreType.DMA((Z,)),
        ],
        compiler_params=pltpu.CompilerParams(vmem_limit_bytes=10 << 20),
        cost_estimate=pl.CostEstimate(flops=8_000_000, bytes_accessed=8_000_000, transcendentals=0),
        name="opened",
    )(in_hbm(w_gate), in_hbm(w_up), in_hbm(router), in_hbm(gain))
    return out, (gate_head, up_head), blocks


def regrouped_kernel(*refs):
    blocks, outs, pieces = refs[:Z], refs[Z : Z + Y], refs[Z + Y]
    held, in_sems, out_sems, piece_sem = refs[Z + Y + 1 :]
    y = lax.rem(lax.axis_index("shard"), Y)
    copies = [pltpu.make_async_copy(blocks[k], held.at[k], in_sems.at[k]) for k in range(Z)]
    for copy in copies:
        copy.start()
    for copy in copies:
        copy.wait()
    copies = [pltpu.make_async_copy(held.at[:, Y * RAW], pieces, piece_sem)] + [
        pltpu.make_async_copy(
            held.at[:, pl.ds(lax.rem(y + t, Y) * RAW, RAW)], outs[t], out_sems.at[t]
        )
        for t in range(Y)
    ]
    for copy in copies:
        copy.start()
    for copy in copies:
        copy.wait()


def regrouped(blocks):
    rest = blocks[0].shape[1:]
    return pl.pallas_call(
        regrouped_kernel,
        in_specs=[IN_HBM] * Z,
        out_specs=[IN_HBM] * (Y + 1),
        out_shape=[pltpu.HBM((Z, RAW, *rest), jnp.float32)] * Y + [pltpu.HBM((Z, *rest), jnp.float32)],
        scratch_shapes=[
            pltpu.VMEM((Z, *blocks[0].shape), jnp.float32),
            pltpu.SemaphoreType.DMA((Z,)),
            pltpu.SemaphoreType.DMA((Y,)),
            pltpu.SemaphoreType.DMA,
        ],
        compiler_params=pltpu.CompilerParams(vmem_limit_bytes=3 << 20),
        cost_estimate=pl.CostEstimate(flops=8_000_000, bytes_accessed=2_000_000, transcendentals=0),
        name="regrouped",
    )(*[in_hbm(b) for b in blocks])


def in_source_order(blocks, held, sems):
    me = lax.axis_index("shard")
    z, y = me // Y, lax.rem(me, Y)
    copies = []
    for t in range(Y):
        for k, shift in enumerate(SHIFTS):
            source = lax.rem(z + Z - shift, Z) * Y + lax.rem(y + Y - t, Y)
            copies.append(pltpu.make_async_copy(blocks[t].at[k], held.at[source], sems.at[t, k]))
    return copies


def rows_kernel(*refs):
    blocks, router, (held, sems) = refs[:Y], refs[Y], refs[Y + 1 :]
    copies = in_source_order(blocks, held, sems)
    for copy in copies:
        copy.start()
    for copy in copies:
        copy.wait()
    for p in range(Y * Z // 2):
        both = jnp.concatenate([held[2 * p][:, :HALF], held[2 * p + 1][:, :HALF]], axis=1)
        router[:, p * LANES : (p + 1) * LANES] = both.astype(jnp.bfloat16)


def router_rows(pieces):
    experts = pieces[0].shape[1]
    return pl.pallas_call(
        rows_kernel,
        in_specs=[IN_HBM] * Y,
        out_specs=IN_VMEM,
        out_shape=pltpu.VMEM((experts, Y * Z * HALF), jnp.bfloat16),
        scratch_shapes=[
            pltpu.VMEM((Y * Z, *pieces[0].shape[1:]), jnp.float32),
            pltpu.SemaphoreType.DMA((Y, Z)),
        ],
        compiler_params=pltpu.CompilerParams(vmem_limit_bytes=1 << 20),
        cost_estimate=pl.CostEstimate(flops=1_000_000, bytes_accessed=300_000, transcendentals=0),
        name="router_rows",
    )(*[in_hbm(b) for b in pieces])


def finished_kernel(*refs):
    blocks, scale, (gate, up), (held, sems) = refs[:Y], refs[Y], refs[Y + 1 : Y + 3], refs[Y + 3 :]
    copies = in_source_order(blocks, held, sems)
    for copy in copies:
        copy.start()
    inverse = 1.0 / scale[...]
    rows, own = inverse.shape[0], inverse.shape[1] // 2
    for copy in copies:
        copy.wait()
    for p in range(Y * Z // 2):
        lanes = slice(p * LANES, (p + 1) * LANES)
        for j in range(RAW):
            first, second = held[2 * p, j], held[2 * p + 1, j]
            place = slice(j * rows, (j + 1) * rows)
            for out, low, column in ((gate, 0, j), (up, HALF, own + j)):
                factor = jnp.broadcast_to(inverse[:, column : column + 1], (rows, LANES))
                both = jnp.concatenate([first[:, low : low + HALF], second[:, low : low + HALF]], axis=1)
                out[place, lanes] = (both * factor).astype(jnp.bfloat16)


def finished(blocks, scale):
    experts = scale.shape[0]
    out = pltpu.VMEM((RAW * experts, Y * Z * HALF), jnp.bfloat16)
    return pl.pallas_call(
        finished_kernel,
        in_specs=[IN_HBM] * Y + [IN_VMEM],
        out_specs=[IN_VMEM] * 2,
        out_shape=[out, out],
        scratch_shapes=[
            pltpu.VMEM((Y * Z, *blocks[0].shape[1:]), jnp.float32),
            pltpu.SemaphoreType.DMA((Y, Z)),
        ],
        compiler_params=pltpu.CompilerParams(vmem_limit_bytes=6 << 20),
        cost_estimate=pl.CostEstimate(flops=8_000_000, bytes_accessed=3_000_000, transcendentals=0),
        name="finished",
    )(*[in_hbm(b) for b in blocks], in_vmem(scale))


def packed_kernel(gate, up, gate_head, up_head, scales, out, tails, held, tail_sems, sems):
    experts, _, width = gate.shape
    size = Y * Z
    loads = [
        [
            pltpu.make_async_copy(w.at[:, :, pl.ds(low, LANES)], tails.at[c, t], tail_sems.at[c, t])
            for t, w in enumerate((gate, up))
        ]
        for c, low in enumerate(range(HEAD, width, LANES))
    ]
    for pair in loads:
        for copy in pair:
            copy.start()
    own = width // size
    parts = [
        [scales[d % Y, :, (d // Y * 2 + t) * own : (d // Y * 2 + t + 1) * own] for d in range(size)]
        for t in range(2)
    ]
    gate_inverse, up_inverse = (1.0 / jnp.concatenate(p, axis=1) for p in parts)
    copies = []
    for c in range(width // LANES):
        columns = slice(c * LANES, (c + 1) * LANES)
        tail = c - HEAD // LANES
        if tail >= 0:
            for copy in loads[tail]:
                copy.wait()
        turned = []
        for e in range(experts):
            if tail < 0:
                parts = gate_head[e, :, columns], up_head[e, :, columns]
            else:
                parts = tails[tail, 0, e], tails[tail, 1, e]
            both = jnp.concatenate(
                [
                    parts[0] * gate_inverse[e : e + 1, columns],
                    parts[1] * up_inverse[e : e + 1, columns],
                ],
                axis=0,
            )
            turned.append(both.astype(jnp.bfloat16).T)
        held[columns] = jnp.swapaxes(jnp.stack(turned), 0, 1)
        while len(copies) < size and (len(copies) + 1) * own <= (c + 1) * LANES:
            d = len(copies)
            rows = pl.ds(d * own + RAW, own - RAW)
            copies.append(pltpu.make_async_copy(held.at[rows], out.at[d], sems.at[d]))
            copies[-1].start()
    for copy in copies:
        copy.wait()


def packed(w_gate, w_up, gate_head, up_head, scales):
    experts, rows, width = w_gate.shape
    size = Y * Z
    return pl.pallas_call(
        packed_kernel,
        in_specs=[IN_HBM] * 2 + [IN_VMEM] * 3,
        out_specs=IN_HBM,
        out_shape=pltpu.HBM((size, width // size - RAW, experts, 2 * rows), jnp.bfloat16),
        scratch_shapes=[
            pltpu.VMEM(((width - HEAD) // LANES, 2, experts, rows, LANES), jnp.float32),
            pltpu.VMEM((width, experts, 2 * rows), jnp.bfloat16),
            pltpu.SemaphoreType.DMA(((width - HEAD) // LANES, 2)),
            pltpu.SemaphoreType.DMA((size,)),
        ],
        compiler_params=pltpu.CompilerParams(vmem_limit_bytes=12 << 20),
        cost_estimate=pl.CostEstimate(flops=8_000_000, bytes_accessed=9_000_000, transcendentals=0),
        name="packed",
    )(in_hbm(w_gate), in_hbm(w_up), in_vmem(gate_head), in_vmem(up_head), in_vmem(scales))


def placed_kernel(arrived, raw_gate, raw_up, gate, up, gate_held, up_held, raw_sems, sems):
    size, total, _ = arrived.shape
    raw = raw_gate.shape[0]
    copies = []
    for t, (part, out) in enumerate(((raw_gate, gate), (raw_up, up))):
        copies.append(pltpu.make_async_copy(part, out.at[pl.ds(0, raw)], raw_sems.at[t]))
        copies[-1].start()
    for c, low in enumerate(range(0, total, PIECE)):
        high = min(low + PIECE, total)
        rows = slice(low, high)
        for p in range(size // 2):
            first, second = arrived[2 * p, rows], arrived[2 * p + 1, rows]
            lanes = slice(p * LANES, (p + 1) * LANES)
            gate_held[rows, lanes] = jnp.concatenate([first[:, :HALF], second[:, :HALF]], axis=-1)
            up_held[rows, lanes] = jnp.concatenate([first[:, HALF:], second[:, HALF:]], axis=-1)
        for t, (held, out) in enumerate(((gate_held, gate), (up_held, up))):
            copies.append(
                pltpu.make_async_copy(
                    held.at[pl.ds(low, high - low)],
                    out.at[pl.ds(raw + low, high - low)],
                    sems.at[c, t],
                )
            )
            copies[-1].start()
    for copy in copies:
        copy.wait()


def placed(arrived, raw_gate, raw_up):
    size, rest, experts, lanes = arrived.shape
    held = (rest * experts, size * HALF)
    shape = ((rest + RAW) * experts, size * HALF)
    out = jax.ShapeDtypeStruct(shape, jnp.bfloat16)
    results = pl.pallas_call(
        placed_kernel,
        in_specs=[IN_VMEM] * 3,
        out_specs=[IN_HBM] * 2,
        out_shape=[out, out],
        scratch_shapes=[
            pltpu.VMEM(held, jnp.bfloat16),
            pltpu.VMEM(held, jnp.bfloat16),
            pltpu.SemaphoreType.DMA((2,)),
            pltpu.SemaphoreType.DMA((pl.cdiv(held[0], PIECE), 2)),
        ],
        compiler_params=pltpu.CompilerParams(vmem_limit_bytes=12 << 20),
        cost_estimate=pl.CostEstimate(flops=4_000_000, bytes_accessed=6_000_000, transcendentals=0),
        name="placed",
    )(in_vmem(arrived.reshape(size, rest * experts, lanes)), in_vmem(raw_gate), in_vmem(raw_up))
    return [r.reshape(rest + RAW, experts, size * HALF) for r in results]


def stored_kernel(held, out, sem):
    copy = pltpu.make_async_copy(held, out, sem)
    copy.start()
    copy.wait()


def stored(x):
    return pl.pallas_call(
        stored_kernel,
        in_specs=[IN_VMEM],
        out_specs=IN_HBM,
        out_shape=jax.ShapeDtypeStruct(x.shape, x.dtype),
        scratch_shapes=[pltpu.SemaphoreType.DMA],
        compiler_params=pltpu.CompilerParams(vmem_limit_bytes=1 << 20),
        cost_estimate=pl.CostEstimate(flops=1_000_000, bytes_accessed=500_000, transcendentals=0),
        name="stored",
    )(in_vmem(x))


def summed_kernel(share, arrived, out, *refs):
    *mine, held, sems = refs
    held[...] = jnp.sum(arrived[...], axis=0) * share
    copies = [pltpu.make_async_copy(held, out.at[i], sems.at[i]) for i in range(out.shape[0])]
    for copy in copies:
        copy.start()
    for ref in mine:
        ref[...] = held[...]
    for copy in copies:
        copy.wait()


def summed(arrived, count, share, mine=False):
    shape = arrived.shape[1:]
    return pl.pallas_call(
        functools.partial(summed_kernel, share),
        in_specs=[IN_VMEM],
        out_specs=[IN_HBM, IN_VMEM][: 1 + mine],
        out_shape=[
            pltpu.HBM((count, *shape), jnp.float32),
            pltpu.VMEM(shape, jnp.float32),
        ][: 1 + mine],
        scratch_shapes=[pltpu.VMEM(shape, jnp.float32), pltpu.SemaphoreType.DMA((count,))],
        compiler_params=pltpu.CompilerParams(vmem_limit_bytes=1 << 20),
        cost_estimate=pl.CostEstimate(flops=1_000_000, bytes_accessed=500_000, transcendentals=0),
        name="summed",
    )(in_vmem(arrived))


def exchanged(parts, groups=None):
    return lax.all_to_all(
        parts, "shard", split_axis=0, concat_axis=0, tiled=True, axis_index_groups=groups
    )


def shifted(x, z_shift, y_shift):
    pairs = [
        (z * Y + y, (z + z_shift) % Z * Y + (y + y_shift) % Y) for z in range(Z) for y in range(Y)
    ]
    return lax.ppermute(x, "shard", pairs)


def on_device(w_gate, w_up, router_weight, router_gain):
    own = w_gate.shape[2] // (Y * Z)
    sums, heads, blocks = opened(w_gate, w_up, router_weight, router_gain)
    sums = exchanged(sums, ALONG_Y)
    (sums,) = summed(sums, Z, 1.0)
    sums = exchanged(sums, ALONG_Z)
    moved = [blocks[0]]
    for k, shift in enumerate(SHIFTS):
        if k:
            moved.append(shifted(blocks[k], shift, 0))
    scales, scale = summed(sums, Y, 1.0 / D_MODEL, mine=True)
    scale = lax.dynamic_slice_in_dim(
        scale, lax.axis_index("shard") // Y * 2 * own, 2 * own, axis=1
    )
    scales = exchanged(scales, ALONG_Y)
    serve = packed(w_gate, w_up, *heads, scales)
    serve = exchanged(serve)
    *moved, pieces = regrouped(moved)
    pieces = [pieces]
    for t in range(1, Y):
        pieces.append(shifted(pieces[0], 0, t))
    for t in range(1, Y):
        moved[t] = shifted(moved[t], 0, t)
    rows = router_rows(pieces)
    router = lax.all_gather(rows, "expert", axis=0, tiled=True)
    router = stored(router)
    raw_gate, raw_up = finished(moved, scale)
    serve_gate, serve_up = placed(serve, raw_gate, raw_up)
    return (
        jnp.transpose(serve_gate, (1, 2, 0)),
        jnp.transpose(serve_up, (1, 2, 0)),
        scale[:, :own],
        scale[:, own:],
        router.T,
    )


def solution(mesh):
    return jax.shard_map(
        on_device,
        mesh=mesh,
        in_specs=(
            P("expert", "shard", None),
            P("expert", "shard", None),
            P("shard", "expert"),
            P("shard"),
        ),
        out_specs=(
            P("expert", None, "shard"),
            P("expert", None, "shard"),
            P("expert", "shard"),
            P("expert", "shard"),
            P(),
        ),
        check_vma=False,
    )
```
